128 devices in a mesh: prompt: 4 (over x), resp: 32 (over y, z, core).
Axes of the slice: x: 4, y: 4, z: 4, core: 2. Of those that a mesh axis runs over, the one named last changes fastest.
Arguments:
- embeddings: bfloat16 [32, 1024, 3584], P('prompt', 'resp'), parts along dimension 0, may hold values from -6 to 6
- head_weight: bfloat16 [3584, 3584], P('resp'), may hold values from -0.0017089844 to 0.0017089844
- valid_mask: int32 [32, 1024], P('prompt', 'resp'), parts along dimension 0, may hold values from 0 to 1, as said below
Outputs:
- preferences: float32 [32, 1024, 1024], P('prompt', 'resp'), parts along dimension 0
- win_rates: float32 [32, 1024], P('prompt', 'resp'), parts along dimension 0
The draws below stay inside these ranges and needn't reach their ends.
There are 4 independent parts, one for each index of `prompt`. The reference program is written for one: setup_inputs(seed, part) draws one part's arguments, and reference() takes and returns one part's arrays. A program takes and returns all parts, laid end to end along the dimension named above; an argument that names none is the same for every part. Nothing has to cross between parts.
Inputs may be any that keep to these rules, and one draw needn't show every extreme that they name: `valid_mask`: for each prompt the ones are its first response slots, between 256 and 1024 of them; in every draw some prompt has all 1024 slots filled.
All inputs are finite; a program needn't handle non-finite values.
Results may differ from the reference program's by a relative error of at most 0.003.
Values may be sent and summed in bfloat16 or wider, within the bound.
No kernel may reach another device: no remote copies, remote signals or barrier semaphores. Data moves between devices by JAX's collectives and lax.ppermute only.
A program may use at most 128 MiB of HBM per device.

```python
import jax
import jax.numpy as jnp
from jax import lax

D = 3584
PROMPTS = 8
RESP = 1024


def draw_valid_mask(key, part):
    first, second, third = jax.random.split(key, 3)
    lengths = jax.random.randint(first, (PROMPTS,), RESP // 4, RESP + 1)
    prompt_ids = jnp.arange(PROMPTS, dtype=jnp.int32)
    shortest = jax.random.randint(second, (), 0, PROMPTS)
    longest = jax.random.randint(third, (), 0, PROMPTS)
    lengths = jnp.where(prompt_ids == shortest, RESP // 4, lengths)
    lengths = jnp.where(prompt_ids == longest, RESP, lengths)
    slot_ids = jnp.arange(RESP, dtype=jnp.int32)
    return (slot_ids[None, :] < lengths[:, None]).astype(jnp.int32)


def block_levels(rng, shape, cuts, smallest, largest):
    loudness = 1.0
    for position, shards_of in cuts:
        steps = jax.random.uniform(jax.random.fold_in(jax.random.fold_in(rng, 6), position), (shards_of,), jnp.float32, smallest / len(cuts), largest / len(cuts))
        loudness = loudness * jnp.repeat(jnp.exp(steps), shape[position] // shards_of).reshape((-1,) + (1,) * (len(shape) - 1 - position))
    return loudness


def noise(stream_key, dims, deviation, most, pieces=(), held_as=jnp.bfloat16):
    drawn = deviation * jax.random.normal(stream_key, dims, jnp.float32)
    if pieces:
        drawn = drawn * block_levels(stream_key, dims, pieces, -0.22, 0.18)
    return jnp.clip(drawn, -most, most).astype(held_as)


def setup_inputs(seed: int = 0, part: int = 0) -> dict:
    keys = jax.random.split(jax.random.key(seed), 4)
    part_keys = jax.random.split(jax.random.fold_in(keys[3], part), 4)
    return {
        "embeddings": noise(part_keys[0], (PROMPTS, RESP, D), 1.0, 6.0, ((1, 32),)),
        "head_weight": noise(keys[1], (D, D), (D * D) ** -0.5, 0.0017089844, ((0, 32),)),
        "valid_mask": draw_valid_mask(jax.random.fold_in(jax.random.fold_in(keys[3], part), 71), part),
    }


def reference(embeddings, head_weight, valid_mask):
    flat_rows = embeddings.reshape(PROMPTS * RESP, D)
    direct = jnp.dot(flat_rows, head_weight, preferred_element_type=jnp.float32)
    mirror = lax.dot_general(flat_rows, head_weight, (((1,), (1,)), ((), ())), preferred_element_type=jnp.float32)
    projected = (direct - mirror).astype(jnp.bfloat16).reshape(PROMPTS, RESP, D)

    def one_prompt(pair):
        rows_in, proj_in = pair
        return -jnp.dot(rows_in, proj_in.T, preferred_element_type=jnp.float32)

    scores = lax.map(one_prompt, (embeddings, projected))
    valid = valid_mask.astype(jnp.float32)
    counts = jnp.sum(valid, axis=1)
    preferences = jax.nn.sigmoid(scores) * valid[:, :, None] * valid[:, None, :]
    totals = jnp.sum(preferences, axis=2) - 0.5 * valid
    win_rates = valid * totals / jnp.maximum(counts - 1.0, 1.0)[:, None]
    return preferences, win_rates
```

```python
import jax
import jax.numpy as jnp
from jax import lax
from jax.sharding import Mesh, PartitionSpec as P

RESP_AXES = ("y", "z", "c")
FILL = 256.0
FILL_TEST = 128.0
HIDDEN = -1e30
HIDDEN_TEST = -1e29


def ring(axis_size, step):
    return [(i, (i + step) % axis_size) for i in range(axis_size)]


def swap_cores(value):
    return lax.ppermute(value, "c", [(0, 1), (1, 0)])


def slab_pairs(first_core):
    pairs = []
    for y in range(4):
        for c in range(2):
            target = y if c == first_core else y ^ 2
            pairs.append((y * 2 + c, target * 2 + y // 2))
    return pairs


def shards(embeddings, head_weight, valid_mask):
    prompts, block_rows, features = embeddings.shape
    quarter = features // 4
    x = lax.axis_index("x")
    y = lax.axis_index("y")
    c = lax.axis_index("c")
    h = y % 2

    slab = lax.dynamic_slice_in_dim(head_weight, (y ^ x) * quarter, quarter, 1)
    part_a = lax.ppermute(slab, ("y", "c"), slab_pairs(0))
    part_b = lax.ppermute(slab, ("y", "c"), slab_pairs(1))
    at_home = c == y // 2
    both = jnp.stack([jnp.where(at_home, part_a, part_b), jnp.where(at_home, part_b, part_a)])
    copies = jnp.broadcast_to(both, (4, *both.shape))
    own = lax.all_to_all(copies, "z", 0, 0, tiled=True).reshape(quarter, quarter)
    half = quarter // 2
    below = lax.ppermute(own, "x", ring(4, 1))
    above = lax.ppermute(own, "x", ring(4, -1))
    across_top = lax.ppermute(below[:half], "x", ring(4, 1))
    across_bottom = lax.ppermute(above[half:], "x", ring(4, -1))
    across = jnp.concatenate([across_top, across_bottom])
    weights = jnp.zeros((4, quarter, quarter), head_weight.dtype)
    for step, piece in ((0, own), (3, below), (1, above), (2, across)):
        weights = lax.dynamic_update_slice_in_dim(weights, piece[None], (x + step) % 4, 0)

    filled = jnp.where(valid_mask[:, :, None] > 0, embeddings, jnp.asarray(FILL, embeddings.dtype))
    grouped = filled.reshape(2, 4, block_rows, 2, 2, quarter)
    grouped = jnp.transpose(grouped, (0, 1, 3, 2, 4, 5))
    outgoing = jnp.stack([grouped, grouped[..., ::-1, :]], axis=1)
    outgoing = outgoing.reshape(32, block_rows, 2 * quarter)
    near = lax.all_to_all(outgoing, RESP_AXES, 0, 0, tiled=True).reshape(32 * block_rows, 2 * quarter)
    far = swap_cores(near)

    def product(index, rows):
        return lax.dot_general(
            weights[index], rows, (((1,), (1,)), ((), ())), preferred_element_type=jnp.float32
        )

    mixed = product(0, near[:, :quarter]) + product(1, near[:, quarter:])
    mixed = mixed + product(2, far[:, :quarter]) + product(3, far[:, quarter:])
    table = jnp.dot(near[:, :quarter], mixed.astype(jnp.bfloat16), preferred_element_type=jnp.float32)
    skew = table - table.T
    slots = 32 * block_rows
    skew = skew.reshape(32, 2, block_rows // 2, slots)
    kept = lax.dynamic_slice_in_dim(skew, c, 1, 1)[:, 0]
    given = lax.dynamic_slice_in_dim(skew, 1 - c, 1, 1)[:, 0].astype(jnp.bfloat16)
    half_scores = kept + swap_cores(given).astype(jnp.float32)
    filled_columns = near[:, 0] < FILL_TEST
    half_scores = jnp.where(filled_columns[None, None, :], half_scores, HIDDEN).astype(jnp.bfloat16)
    returned = lax.all_to_all(half_scores, RESP_AXES, 0, 0, tiled=True)
    returned = returned.astype(jnp.float32).reshape(2, 2, 4, 2, block_rows // 2, slots)
    scores = (returned[:, 0] + returned[:, 1]).reshape(prompts, block_rows, slots)

    valid_rows = valid_mask.astype(jnp.float32)
    counts = jnp.sum((scores > HIDDEN_TEST).astype(jnp.float32), axis=2)
    preferences = jax.nn.sigmoid(scores) * valid_rows[:, :, None]
    totals = jnp.sum(preferences, axis=2) - 0.5 * valid_rows
    win_rates = valid_rows * totals / jnp.maximum(counts - 1.0, 1.0)
    return preferences, win_rates


def solution(mesh):
    mesh = Mesh(mesh.devices.reshape(4, 4, 4, 2), ("x", "y", "z", "c"))
    spec = P("x", RESP_AXES)
    return jax.shard_map(
        shards,
        mesh=mesh,
        in_specs=(P("x", RESP_AXES, None), P(RESP_AXES, None), spec),
        out_specs=(P("x", RESP_AXES, None), spec),
        check_vma=False,
    )
```

```python
import jax
import jax.numpy as jnp
from jax import lax
from jax.experimental import pallas as pl
from jax.experimental.pallas import tpu as pltpu
from jax.sharding import Mesh, PartitionSpec as P


RESP_AXES = ("y", "z", "c")
FILL = 256.0
FILL_TEST = 128.0
HIDDEN = 1e30
HIDDEN_TEST = -1e29


def ring(value, axis, step):
    return lax.ppermute(value, axis, [(i, (i + step) % 4) for i in range(4)])


def swap_cores(value):
    return lax.ppermute(value, "c", [(0, 1), (1, 0)])


def slab_pairs(first_core):
    pairs = []
    for y in range(4):
        for c in range(2):
            target = y if c == first_core else y ^ 2
            pairs.append((y * 2 + c, target * 2 + y // 2))
    return pairs


def pack_kernel(rows_ref, valid_ref, out_ref):
    rows = rows_ref[0]
    filled = jnp.where(valid_ref[0] > 0, rows, jnp.asarray(FILL, rows.dtype))
    half = filled.shape[1] // 2
    quarter = half // 2
    for c in range(2):
        lanes = filled[:, c * half : (c + 1) * half]
        out_ref[0, 0, 0, c] = lanes
        out_ref[0, 1, 0, c, :, :quarter] = lanes[:, quarter:]
        out_ref[0, 1, 0, c, :, quarter:] = lanes[:, :quarter]


def pack(embeddings, valid_mask):
    prompts, block_rows, features = embeddings.shape
    half = features // 2
    out = pl.pallas_call(
        pack_kernel,
        grid=(prompts,),
        in_specs=[
            pl.BlockSpec((1, block_rows, features), lambda p: (p, 0, 0)),
            pl.BlockSpec((1, block_rows, 1), lambda p: (p, 0, 0)),
        ],
        out_specs=pl.BlockSpec((1, 2, 1, 2, block_rows, half), lambda p: (p // 4, 0, p % 4, 0, 0, 0)),
        out_shape=jax.ShapeDtypeStruct((2, 2, 4, 2, block_rows, half), embeddings.dtype),
    )(embeddings, valid_mask[:, :, None])
    return out.reshape(32, block_rows, half)


def load_weights(place_ref, pieces, w_ref, sems, first):
    quarter = w_ref.shape[0]
    rows = quarter // 4
    for s in range(4):
        position = lax.rem(place_ref[0] + s, 4)

        @pl.when(jnp.logical_and(position >= first, position < first + 2))
        def _():
            for r in range(4):
                at = pl.multiple_of(lax.rem(place_ref[1] + r, 4) * rows, rows)
                lanes = pl.multiple_of((position - first) * quarter, quarter)
                pltpu.make_async_copy(
                    pieces[s * 4 + r], w_ref.at[pl.ds(at, rows), pl.ds(lanes, quarter)], sems.at[s * 4 + r]
                ).start()


def wait_weights(place_ref, pieces, w_ref, sems, first):
    quarter = w_ref.shape[0]
    rows = quarter // 4
    for s in range(4):
        position = lax.rem(place_ref[0] + s, 4)

        @pl.when(jnp.logical_and(position >= first, position < first + 2))
        def _():
            for r in range(4):
                at = pl.multiple_of(lax.rem(place_ref[1] + r, 4) * rows, rows)
                lanes = pl.multiple_of((position - first) * quarter, quarter)
                pltpu.make_async_copy(
                    pieces[s * 4 + r], w_ref.at[pl.ds(at, rows), pl.ds(lanes, quarter)], sems.at[s * 4 + r]
                ).wait()


def times_rows(w_ref, rows_ref):
    return lax.dot_general(
        w_ref[...], rows_ref[...], (((1,), (1,)), ((), ())), preferred_element_type=jnp.float32
    )


def near_kernel(place_ref, near_ref, *refs):
    pieces, mixed_ref, w_ref, sems = refs[:16], refs[16], refs[17], refs[18]
    load_weights(place_ref, pieces, w_ref, sems, 0)
    wait_weights(place_ref, pieces, w_ref, sems, 0)
    mixed_ref[...] = times_rows(w_ref, near_ref)


def far_kernel(place_ref, near_ref, far_ref, mixed_ref, *refs):
    pieces, kept_ref, given_ref, w_ref, total_ref, table_ref, sems = refs[:16], *refs[16:]
    load_weights(place_ref, pieces, w_ref, sems, 2)
    wait_weights(place_ref, pieces, w_ref, sems, 2)
    total_ref[...] = (mixed_ref[...] + times_rows(w_ref, far_ref)).astype(total_ref.dtype)
    quarter = w_ref.shape[0]
    slots = table_ref.shape[0]
    hidden = jnp.where(near_ref[:, :1].astype(jnp.float32) < FILL_TEST, 0.0, HIDDEN)
    table_ref[...] = (
        jnp.dot(near_ref[:, :quarter], total_ref[...], preferred_element_type=jnp.float32) + hidden
    )
    c = place_ref[2]
    block = 128
    part = kept_ref.shape[1]
    for i in range(slots // block):
        rows = slice(i * block, (i + 1) * block)
        skew = table_ref[rows, :] - table_ref[:, rows].T
        groups = block // (2 * part)
        skew = skew.reshape(groups, 2, part, slots)
        first, second = skew[:, 0], skew[:, 1]
        at = slice(i * groups, (i + 1) * groups)
        kept_ref[at] = jnp.where(c == 0, first, second)
        given_ref[at] = jnp.where(c == 0, second, first).astype(given_ref.dtype)


def in_hbm():
    return pl.BlockSpec(memory_space=pl.ANY)


def whole():
    return pl.BlockSpec(memory_space=pltpu.VMEM)


def score_parts(place, near, far, pieces):
    slots, half = near.shape
    quarter = half // 2
    scalars = pl.BlockSpec(memory_space=pltpu.SMEM)
    limit = pltpu.CompilerParams(vmem_limit_bytes=56 * 2**20)
    mixed = pl.pallas_call(
        near_kernel,
        in_specs=[scalars, whole()] + [in_hbm()] * 16,
        out_specs=whole(),
        out_shape=jax.ShapeDtypeStruct((quarter, slots), jnp.float32),
        scratch_shapes=[pltpu.VMEM((quarter, half), near.dtype), pltpu.SemaphoreType.DMA((16,))],
        compiler_params=limit,
        cost_estimate=pl.CostEstimate(
            flops=2 * quarter * half * slots, bytes_accessed=12 * 2**20, transcendentals=0
        ),
    )(place, near, *pieces)
    part = slots // 64
    return pl.pallas_call(
        far_kernel,
        in_specs=[scalars, whole(), whole(), whole()] + [in_hbm()] * 16,
        out_specs=[whole(), whole()],
        out_shape=[
            jax.ShapeDtypeStruct((32, part, slots), jnp.float32),
            jax.ShapeDtypeStruct((32, part, slots), jnp.bfloat16),
        ],
        scratch_shapes=[
            pltpu.VMEM((quarter, half), near.dtype),
            pltpu.VMEM((quarter, slots), near.dtype),
            pltpu.VMEM((slots, slots), jnp.float32),
            pltpu.SemaphoreType.DMA((16,)),
        ],
        compiler_params=limit,
        cost_estimate=pl.CostEstimate(
            flops=2 * quarter * (half + slots) * slots, bytes_accessed=16 * 2**20, transcendentals=0
        ),
    )(place, near, far, mixed, *pieces)


def scored(embeddings, head_weight, valid_mask):
    prompts, block_rows, features = embeddings.shape
    quarter = features // 4
    slots = 32 * block_rows
    x = lax.axis_index("x")
    y = lax.axis_index("y")
    z = lax.axis_index("z")
    c = lax.axis_index("c")

    slab = lax.dynamic_slice_in_dim(head_weight, (y ^ x) * quarter, quarter, 1)
    part_a = lax.ppermute(slab, ("y", "c"), slab_pairs(0))
    part_b = lax.ppermute(slab, ("y", "c"), slab_pairs(1))
    outgoing = pack(embeddings, valid_mask)
    at_home = c == y // 2
    own = jnp.concatenate([jnp.where(at_home, part_a, part_b), jnp.where(at_home, part_b, part_a)])
    chain = [own, ring(own, "z", -1), ring(own, "z", 2), ring(own, "z", 1)]
    near = lax.all_to_all(outgoing, RESP_AXES, 0, 0, tiled=True).reshape(slots, 2 * quarter)
    below, above = [], []
    for piece in chain:
        below.append(ring(piece, "x", 1))
        above.append(ring(piece, "x", -1))
    across = [
        ring(below[0], "x", 1),
        ring(above[1], "x", -1),
        ring(above[2], "x", -1),
        ring(below[3], "x", 1),
    ]
    far = swap_cores(near)

    place = jnp.stack([x, z, c]).astype(jnp.int32)
    kept, given = score_parts(place, near, far, [*chain, *above, *across, *below])
    half_scores = (kept + swap_cores(given).astype(jnp.float32)).astype(jnp.bfloat16)
    returned = lax.all_to_all(half_scores, RESP_AXES, 0, 0, tiled=True)
    returned = returned.astype(jnp.float32).reshape(2, 2, 4, 2, block_rows // 2, slots)
    scores = (returned[:, 0] + returned[:, 1]).reshape(prompts, block_rows, slots)

    valid_rows = valid_mask.astype(jnp.float32)
    counts = jnp.sum((scores > HIDDEN_TEST).astype(jnp.float32), axis=2)
    preferences = jax.nn.sigmoid(scores) * valid_rows[:, :, None]
    totals = jnp.sum(preferences, axis=2) - 0.5 * valid_rows
    win_rates = valid_rows * totals / jnp.maximum(counts - 1.0, 1.0)
    return preferences, win_rates


def solution(mesh):
    mesh = Mesh(mesh.devices.reshape(4, 4, 4, 2), ("x", "y", "z", "c"))
    spec = P("x", RESP_AXES)
    return jax.shard_map(
        scored,
        mesh=mesh,
        in_specs=(P("x", RESP_AXES, None), P(RESP_AXES, None), spec),
        out_specs=(P("x", RESP_AXES, None), spec),
        check_vma=False,
    )
```

```python
import jax
import jax.numpy as jnp
from jax import lax
from jax.experimental import pallas as pl
from jax.experimental.pallas import tpu as pltpu
from jax.sharding import Mesh, PartitionSpec as P


RESP_AXES = ("y", "z", "c")
FILL = 256.0
FILL_TEST = 128.0
HIDDEN = 1e30
HIDDEN_TEST = -1e29


def ring(value, axis, step):
    return lax.ppermute(value, axis, [(i, (i + step) % 4) for i in range(4)])


def swap_cores(value):
    return lax.ppermute(value, "c", [(0, 1), (1, 0)])


def slab_pairs(first_core):
    pairs = []
    for y in range(4):
        for c in range(2):
            target = y if c == first_core else y ^ 2
            pairs.append((y * 2 + c, target * 2 + y // 2))
    return pairs


def pack_kernel(rows_ref, valid_ref, out_ref):
    rows = rows_ref[0]
    filled = jnp.where(valid_ref[0] > 0, rows, jnp.asarray(FILL, rows.dtype))
    half = filled.shape[1] // 2
    quarter = half // 2
    for c in range(2):
        lanes = filled[:, c * half : (c + 1) * half]
        out_ref[0, 0, 0, c] = lanes
        out_ref[0, 1, 0, c, :, :quarter] = lanes[:, quarter:]
        out_ref[0, 1, 0, c, :, quarter:] = lanes[:, :quarter]


def pack(embeddings, valid_mask):
    prompts, block_rows, features = embeddings.shape
    half = features // 2
    out = pl.pallas_call(
        pack_kernel,
        grid=(prompts,),
        in_specs=[
            pl.BlockSpec((1, block_rows, features), lambda p: (p, 0, 0)),
            pl.BlockSpec((1, block_rows, 1), lambda p: (p, 0, 0)),
        ],
        out_specs=pl.BlockSpec((1, 2, 1, 2, block_rows, half), lambda p: (p // 4, 0, p % 4, 0, 0, 0)),
        out_shape=jax.ShapeDtypeStruct((2, 2, 4, 2, block_rows, half), embeddings.dtype),
    )(embeddings, valid_mask[:, :, None])
    return out.reshape(32, block_rows, half)


def load_weights(place_ref, pieces, w_ref, sems, first):
    quarter = w_ref.shape[0]
    rows = quarter // 4
    for s in range(4):
        position = lax.rem(place_ref[0] + s, 4)

        @pl.when(jnp.logical_and(position >= first, position < first + 2))
        def _():
            for r in range(4):
                at = pl.multiple_of(lax.rem(place_ref[1] + r, 4) * rows, rows)
                lanes = pl.multiple_of((position - first) * quarter, quarter)
                pltpu.make_async_copy(
                    pieces[s * 4 + r], w_ref.at[pl.ds(at, rows), pl.ds(lanes, quarter)], sems.at[s * 4 + r]
                ).start()


def wait_weights(place_ref, pieces, w_ref, sems, first):
    quarter = w_ref.shape[0]
    rows = quarter // 4
    for s in range(4):
        position = lax.rem(place_ref[0] + s, 4)

        @pl.when(jnp.logical_and(position >= first, position < first + 2))
        def _():
            for r in range(4):
                at = pl.multiple_of(lax.rem(place_ref[1] + r, 4) * rows, rows)
                lanes = pl.multiple_of((position - first) * quarter, quarter)
                pltpu.make_async_copy(
                    pieces[s * 4 + r], w_ref.at[pl.ds(at, rows), pl.ds(lanes, quarter)], sems.at[s * 4 + r]
                ).wait()


def times_rows(w_ref, rows_ref):
    return lax.dot_general(
        w_ref[...], rows_ref[...], (((1,), (1,)), ((), ())), preferred_element_type=jnp.float32
    )


def near_kernel(place_ref, near_ref, *refs):
    pieces, mixed_ref, w_ref, sems = refs[:16], refs[16], refs[17], refs[18]
    load_weights(place_ref, pieces, w_ref, sems, 0)
    wait_weights(place_ref, pieces, w_ref, sems, 0)
    mixed_ref[...] = times_rows(w_ref, near_ref)


def far_kernel(place_ref, near_ref, far_ref, mixed_ref, *refs):
    pieces, kept_ref, given_ref, w_ref, total_ref, table_ref, sems = refs[:16], *refs[16:]
    load_weights(place_ref, pieces, w_ref, sems, 2)
    wait_weights(place_ref, pieces, w_ref, sems, 2)
    total_ref[...] = (mixed_ref[...] + times_rows(w_ref, far_ref)).astype(total_ref.dtype)
    quarter = w_ref.shape[0]
    slots = table_ref.shape[0]
    hidden = jnp.where(near_ref[:, :1].astype(jnp.float32) < FILL_TEST, 0.0, HIDDEN)
    table_ref[...] = (
        jnp.dot(near_ref[:, :quarter], total_ref[...], preferred_element_type=jnp.float32) + hidden
    )
    c = place_ref[2]
    block = 128
    part = kept_ref.shape[1]
    for i in range(slots // block):
        rows = slice(i * block, (i + 1) * block)
        skew = table_ref[rows, :] - table_ref[:, rows].T
        groups = block // (2 * part)
        skew = skew.reshape(groups, 2, part, slots)
        first, second = skew[:, 0], skew[:, 1]
        at = slice(i * groups, (i + 1) * groups)
        kept_ref[at] = jnp.where(c == 0, first, second)
        given_ref[at] = jnp.where(c == 0, second, first).astype(given_ref.dtype)


def in_hbm():
    return pl.BlockSpec(memory_space=pl.ANY)


def whole():
    return pl.BlockSpec(memory_space=pltpu.VMEM)


def score_parts(place, near, far, pieces):
    slots, half = near.shape
    quarter = half // 2
    scalars = pl.BlockSpec(memory_space=pltpu.SMEM)
    limit = pltpu.CompilerParams(vmem_limit_bytes=56 * 2**20)
    mixed = pl.pallas_call(
        near_kernel,
        in_specs=[scalars, whole()] + [in_hbm()] * 16,
        out_specs=whole(),
        out_shape=jax.ShapeDtypeStruct((quarter, slots), jnp.float32),
        scratch_shapes=[pltpu.VMEM((quarter, half), near.dtype), pltpu.SemaphoreType.DMA((16,))],
        compiler_params=limit,
        cost_estimate=pl.CostEstimate(
            flops=2 * quarter * half * slots, bytes_accessed=12 * 2**20, transcendentals=0
        ),
    )(place, near, *pieces)
    part = slots // 64
    return pl.pallas_call(
        far_kernel,
        in_specs=[scalars, whole(), whole(), whole()] + [in_hbm()] * 16,
        out_specs=[whole(), whole()],
        out_shape=[
            jax.ShapeDtypeStruct((32, part, slots), jnp.float32),
            jax.ShapeDtypeStruct((32, part, slots), jnp.bfloat16),
        ],
        scratch_shapes=[
            pltpu.VMEM((quarter, half), near.dtype),
            pltpu.VMEM((quarter, slots), near.dtype),
            pltpu.VMEM((slots, slots), jnp.float32),
            pltpu.SemaphoreType.DMA((16,)),
        ],
        compiler_params=limit,
        cost_estimate=pl.CostEstimate(
            flops=2 * quarter * (half + slots) * slots, bytes_accessed=16 * 2**20, transcendentals=0
        ),
    )(place, near, far, mixed, *pieces)


def scored(embeddings, head_weight, valid_mask):
    prompts, block_rows, features = embeddings.shape
    quarter = features // 4
    slots = 32 * block_rows
    x = lax.axis_index("x")
    y = lax.axis_index("y")
    z = lax.axis_index("z")
    c = lax.axis_index("c")

    slab = lax.dynamic_slice_in_dim(head_weight, (y ^ x) * quarter, quarter, 1)
    part_a = lax.ppermute(slab, ("y", "c"), slab_pairs(0))
    part_b = lax.ppermute(slab, ("y", "c"), slab_pairs(1))
    outgoing = pack(embeddings, valid_mask)
    at_home = c == y // 2
    own = jnp.concatenate([jnp.where(at_home, part_a, part_b), jnp.where(at_home, part_b, part_a)])
    chain = [own, ring(own, "z", -1), ring(own, "z", 2), ring(own, "z", 1)]
    near = lax.all_to_all(outgoing, RESP_AXES, 0, 0, tiled=True).reshape(slots, 2 * quarter)
    below, above = [], []
    for piece in chain:
        below.append(ring(piece, "x", 1))
        above.append(ring(piece, "x", -1))
    across = []
    for index, step in enumerate((1, -1, -1, 1)):
        across.append(ring((below if step == 1 else above)[index], "x", step))
    far = swap_cores(near)

    place = jnp.stack([x, z, c]).astype(jnp.int32)
    kept, given = score_parts(place, near, far, [*chain, *above, *across, *below])
    half_scores = (kept + swap_cores(given).astype(jnp.float32)).astype(jnp.bfloat16)
    returned = lax.all_to_all(half_scores, RESP_AXES, 0, 0, tiled=True)
    returned = returned.astype(jnp.float32).reshape(2, 2, 4, 2, block_rows // 2, slots)
    scores = (returned[:, 0] + returned[:, 1]).reshape(prompts, block_rows, slots)

    valid_rows = valid_mask.astype(jnp.float32)
    counts = jnp.sum((scores > HIDDEN_TEST).astype(jnp.float32), axis=2)
    preferences = jax.nn.sigmoid(scores) * valid_rows[:, :, None]
    totals = jnp.sum(preferences, axis=2) - 0.5 * valid_rows
    win_rates = valid_rows * totals / jnp.maximum(counts - 1.0, 1.0)
    return preferences, win_rates


def solution(mesh):
    mesh = Mesh(mesh.devices.reshape(4, 4, 4, 2), ("x", "y", "z", "c"))
    spec = P("x", RESP_AXES)
    return jax.shard_map(
        scored,
        mesh=mesh,
        in_specs=(P("x", RESP_AXES, None), P(RESP_AXES, None), spec),
        out_specs=(P("x", RESP_AXES, None), spec),
        check_vma=False,
    )
```

```python
import jax
import jax.numpy as jnp
from jax import lax
from jax.experimental import pallas as pl
from jax.experimental.pallas import tpu as pltpu
from jax.sharding import Mesh, PartitionSpec as P


RESP_AXES = ("y", "z", "c")
FILL = 256.0
FILL_TEST = 128.0
HIDDEN = 1e30
HIDDEN_TEST = -1e29
CHUNKS = 2
PIECES = tuple((s, r, 0) for s in (0, 1, 3) for r in range(4)) + ((2, 0, 0), (2, 1, 0), (2, 2, 0), (2, 2, 1), (2, 3, 0))
COUNT = len(PIECES)


def ring(value, axis, step):
    return lax.ppermute(value, axis, [(i, (i + step) % 4) for i in range(4)])


def swap_cores(value):
    return lax.ppermute(value, "c", [(0, 1), (1, 0)])


def slab_pairs(first_core):
    pairs = []
    for y in range(4):
        for c in range(2):
            target = y if c == first_core else y ^ 1
            pairs.append((y * 2 + c, target * 2 + y % 2))
    return pairs


def pack_kernel(rows_ref, valid_ref, out_ref, in_ref, send_ref, in_sems, out_sems):
    prompts, _, features = in_ref.shape
    half = features // 2
    quarter = half // 2
    loads = [
        pltpu.make_async_copy(rows_ref.at[p], in_ref.at[p], in_sems.at[p]) for p in range(prompts)
    ]
    stores = [
        pltpu.make_async_copy(send_ref.at[p], out_ref.at[:, p // 4, p % 4], out_sems.at[p])
        for p in range(prompts)
    ]
    for load in loads:
        load.start()
    valid = valid_ref[...].astype(jnp.float32).T
    for p in range(prompts):
        loads[p].wait()
        rows = in_ref[p]
        filled = jnp.where(valid[:, p : p + 1] > 0, rows.astype(jnp.float32), FILL).astype(rows.dtype)
        for h in range(2):
            for c in range(2):
                for place, index in enumerate((2 * h + c, 2 * (1 - h) + c)):
                    send_ref[p, h, c, :, place * quarter : (place + 1) * quarter] = filled[
                        :, index * quarter : (index + 1) * quarter
                    ]
        stores[p].start()
    for store in stores:
        store.wait()


def pack(embeddings, valid_mask):
    prompts, block_rows, features = embeddings.shape
    half = features // 2
    out = pl.pallas_call(
        pack_kernel,
        in_specs=[in_hbm(), whole()],
        out_specs=in_hbm(),
        out_shape=jax.ShapeDtypeStruct((2, 2, 4, 2, block_rows, half), embeddings.dtype),
        scratch_shapes=[
            pltpu.VMEM(embeddings.shape, embeddings.dtype),
            pltpu.VMEM((prompts, 2, 2, block_rows, half), embeddings.dtype),
            pltpu.SemaphoreType.DMA((prompts,)),
            pltpu.SemaphoreType.DMA((prompts,)),
        ],
    )(embeddings, valid_mask)
    return out.reshape(32, block_rows, half)


def weight_copies(place_ref, pieces, w_ref, sems, first, s):
    quarter = w_ref.shape[0]
    rows = quarter // 4
    position = lax.rem(place_ref[0] + s, 4)
    lanes = pl.multiple_of((position - first) * quarter, quarter)
    copies = []
    for index, (from_plane, from_row, half) in enumerate(PIECES):
        if from_plane == s:
            count = pieces[index].shape[0]
            at = pl.multiple_of(lax.rem(place_ref[1] + from_row, 4) * rows + half * count, count)
            target = w_ref.at[pl.ds(at, count), pl.ds(lanes, quarter)]
            copies.append(pltpu.make_async_copy(pieces[index], target, sems.at[index]))
    return jnp.logical_and(position >= first, position < first + 2), copies


def load_weights(place_ref, pieces, w_ref, sems, first):
    for s in range(4):
        here, copies = weight_copies(place_ref, pieces, w_ref, sems, first, s)

        @pl.when(here)
        def _():
            for copy in copies:
                copy.start()


def wait_weights(place_ref, pieces, w_ref, sems, first):
    for s in range(4):
        here, copies = weight_copies(place_ref, pieces, w_ref, sems, first, s)

        @pl.when(here)
        def _():
            for copy in copies:
                copy.wait()


def times_rows(w_ref, rows):
    return lax.dot_general(w_ref[...], rows, (((1,), (1,)), ((), ())), preferred_element_type=jnp.float32)


def row_loads(source, target, sems):
    rows = target.shape[0] // CHUNKS
    at = [pl.ds(n * rows, rows) for n in range(CHUNKS)]
    return [pltpu.make_async_copy(source.at[at[n]], target.at[at[n]], sems.at[n]) for n in range(CHUNKS)]


def near_kernel(place_ref, near_hbm, *refs):
    pieces, (mixed_hbm, w_ref, near_ref, mixed_ref, sems, near_sems, out_sems) = refs[:COUNT], refs[COUNT:]
    load_weights(place_ref, pieces, w_ref, sems, 0)
    loads = row_loads(near_hbm, near_ref, near_sems)
    for load in loads:
        load.start()
    wait_weights(place_ref, pieces, w_ref, sems, 0)
    rows = near_ref.shape[0] // CHUNKS
    stores = []
    for n in range(CHUNKS):
        loads[n].wait()
        mixed_ref[n] = times_rows(w_ref, near_ref[n * rows : (n + 1) * rows, :])
        stores.append(pltpu.make_async_copy(mixed_ref.at[n], mixed_hbm.at[n], out_sems.at[n]))
        stores[n].start()
    for store in stores:
        store.wait()


def far_kernel(place_ref, near_hbm, far_hbm, mixed_hbm, *refs):
    pieces, outs, scratch = refs[:COUNT], refs[COUNT : COUNT + 2], refs[COUNT + 2 :]
    kept_ref, given_ref = outs
    w_ref, far_ref, first_ref, mixed_ref, total_ref, table_ref, sems, far_sems, mixed_sems, first_sem = scratch
    load_weights(place_ref, pieces, w_ref, sems, 2)
    quarter = w_ref.shape[0]
    slots = table_ref.shape[0]
    rows = slots // CHUNKS
    loads = row_loads(far_hbm, far_ref, far_sems)
    partials = [pltpu.make_async_copy(mixed_hbm.at[n], mixed_ref.at[n], mixed_sems.at[n]) for n in range(CHUNKS)]
    first = pltpu.make_async_copy(near_hbm.at[:, pl.ds(0, quarter)], first_ref, first_sem.at[0])
    for n in range(CHUNKS):
        loads[n].start()
        partials[n].start()
    first.start()
    wait_weights(place_ref, pieces, w_ref, sems, 2)
    for n in range(CHUNKS):
        at = slice(n * rows, (n + 1) * rows)
        loads[n].wait()
        partials[n].wait()
        total_ref[:, at] = (mixed_ref[n] + times_rows(w_ref, far_ref[at, :])).astype(total_ref.dtype)
    first.wait()
    hidden = jnp.where(first_ref[:, :1].astype(jnp.float32) < FILL_TEST, 0.0, HIDDEN)
    table_ref[...] = jnp.dot(first_ref[...], total_ref[...], preferred_element_type=jnp.float32) + hidden
    c = place_ref[2]
    block = 128
    part = kept_ref.shape[1]
    for i in range(slots // block):
        at = slice(i * block, (i + 1) * block)
        skew = table_ref[at, :] - table_ref[:, at].T
        groups = block // (2 * part)
        skew = skew.reshape(groups, 2, part, slots)
        low, high = skew[:, 0], skew[:, 1]
        at = slice(i * groups, (i + 1) * groups)
        kept_ref[at] = jnp.where(c == 0, low, high).astype(kept_ref.dtype)
        given_ref[at] = jnp.where(c == 0, high, low).astype(given_ref.dtype)


def in_hbm():
    return pl.BlockSpec(memory_space=pl.ANY)


def whole():
    return pl.BlockSpec(memory_space=pltpu.VMEM)


def score_parts(place, near, far, pieces):
    slots, half = near.shape
    quarter = half // 2
    rows = slots // CHUNKS
    scalars = pl.BlockSpec(memory_space=pltpu.SMEM)
    limit = pltpu.CompilerParams(vmem_limit_bytes=56 * 2**20)
    four = pltpu.SemaphoreType.DMA((CHUNKS,))
    each = pltpu.SemaphoreType.DMA((COUNT,))
    mixed = pl.pallas_call(
        near_kernel,
        in_specs=[scalars] + [in_hbm()] * (COUNT + 1),
        out_specs=in_hbm(),
        out_shape=jax.ShapeDtypeStruct((CHUNKS, quarter, rows), jnp.float32),
        scratch_shapes=[
            pltpu.VMEM((quarter, half), near.dtype),
            pltpu.VMEM((slots, half), near.dtype),
            pltpu.VMEM((CHUNKS, quarter, rows), jnp.float32),
            each,
            four,
            four,
        ],
        compiler_params=limit,
        cost_estimate=pl.CostEstimate(
            flops=2 * quarter * half * slots, bytes_accessed=12 * 2**20, transcendentals=0
        ),
    )(place, near, *pieces)
    part = slots // 64
    return pl.pallas_call(
        far_kernel,
        in_specs=[scalars] + [in_hbm()] * (COUNT + 3),
        out_specs=[whole(), whole()],
        out_shape=[
            jax.ShapeDtypeStruct((32, part, slots), jnp.bfloat16),
            jax.ShapeDtypeStruct((32, part, slots), jnp.bfloat16),
        ],
        scratch_shapes=[
            pltpu.VMEM((quarter, half), near.dtype),
            pltpu.VMEM((slots, half), near.dtype),
            pltpu.VMEM((slots, quarter), near.dtype),
            pltpu.VMEM((CHUNKS, quarter, rows), jnp.float32),
            pltpu.VMEM((quarter, slots), near.dtype),
            pltpu.VMEM((slots, slots), jnp.float32),
            each,
            four,
            four,
            pltpu.SemaphoreType.DMA((1,)),
        ],
        compiler_params=limit,
        cost_estimate=pl.CostEstimate(
            flops=2 * quarter * (half + slots) * slots, bytes_accessed=16 * 2**20, transcendentals=0
        ),
    )(place, near, far, mixed, *pieces)


def scored(embeddings, head_weight, valid_mask):
    prompts, block_rows, features = embeddings.shape
    quarter = features // 4
    slots = 32 * block_rows
    x = lax.axis_index("x")
    y = lax.axis_index("y")
    z = lax.axis_index("z")
    c = lax.axis_index("c")

    slab = lax.dynamic_slice_in_dim(head_weight, (y ^ ((x % 2) * 2 + x // 2)) * quarter, quarter, 1)
    part_a = lax.ppermute(slab, ("y", "c"), slab_pairs(0))
    part_b = lax.ppermute(slab, ("y", "c"), slab_pairs(1))
    outgoing = pack(embeddings, valid_mask)
    at_home = c == y % 2
    own = jnp.concatenate([jnp.where(at_home, part_a, part_b), jnp.where(at_home, part_b, part_a)])
    chain = [own]
    for step in (-1, 2, 1):
        chain.append(ring(own, "z", step))
    near = lax.all_to_all(outgoing, RESP_AXES, 0, 0, tiled=True).reshape(slots, 2 * quarter)
    below, above = [], []
    for piece in chain:
        below.append(ring(piece, "x", 1))
        above.append(ring(piece, "x", -1))
    across = []
    for index, steps in enumerate(((1,), (-1,), (1, -1), (1,))):
        for half, step in enumerate(steps):
            piece = (below if step == 1 else above)[index]
            rows = piece.shape[0] // len(steps)
            across.append(ring(piece[half * rows : (half + 1) * rows], "x", step))
    far = swap_cores(near)

    place = jnp.stack([x, z, c]).astype(jnp.int32)
    kept, given = score_parts(place, near, far, [*chain, *above, *below, *across])
    half_scores = (kept.astype(jnp.float32) + swap_cores(given).astype(jnp.float32)).astype(jnp.bfloat16)
    returned = lax.all_to_all(half_scores, RESP_AXES, 0, 0, tiled=True)
    returned = returned.astype(jnp.float32).reshape(2, 2, 4, 2, block_rows // 2, slots)
    scores = (returned[0] + returned[1]).reshape(prompts, block_rows, slots)

    valid_rows = valid_mask.astype(jnp.float32)
    counts = jnp.sum((scores > HIDDEN_TEST).astype(jnp.float32), axis=2)
    preferences = jax.nn.sigmoid(scores) * valid_rows[:, :, None]
    totals = jnp.sum(preferences, axis=2) - 0.5 * valid_rows
    win_rates = valid_rows * totals / jnp.maximum(counts - 1.0, 1.0)
    return preferences, win_rates


def solution(mesh):
    mesh = Mesh(mesh.devices.reshape(4, 4, 4, 2), ("x", "y", "z", "c"))
    spec = P("x", RESP_AXES)
    return jax.shard_map(
        scored,
        mesh=mesh,
        in_specs=(P("x", RESP_AXES, None), P(RESP_AXES, None), spec),
        out_specs=(P("x", RESP_AXES, None), spec),
        check_vma=False,
    )
```

```python
import jax
import jax.numpy as jnp
from jax import lax
from jax.experimental import pallas as pl
from jax.experimental.pallas import tpu as pltpu
from jax.sharding import Mesh, PartitionSpec as P


RESP_AXES = ("y", "z", "c")
FILL = 256.0
FILL_TEST = 128.0
HIDDEN = 1e30
HIDDEN_TEST = -1e29
CHUNKS = 2
PIECES = tuple((s, r, 0) for s in (0, 1, 3) for r in range(4)) + ((2, 0, 0), (2, 1, 0), (2, 2, 0), (2, 2, 1), (2, 3, 0))
COUNT = len(PIECES)


def ring(value, axis, step):
    return lax.ppermute(value, axis, [(i, (i + step) % 4) for i in range(4)])


def swap_cores(value):
    return lax.ppermute(value, "c", [(0, 1), (1, 0)])


def slab_pairs(first_core):
    pairs = []
    for y in range(4):
        for c in range(2):
            target = y if c == first_core else y ^ 1
            pairs.append((y * 2 + c, target * 2 + y % 2))
    return pairs


def pack_kernel(rows_ref, valid_ref, out_ref, in_ref, send_ref, in_sems, out_sems):
    prompts, _, features = in_ref.shape
    half = features // 2
    quarter = half // 2
    loads = [
        pltpu.make_async_copy(rows_ref.at[p], in_ref.at[p], in_sems.at[p]) for p in range(prompts)
    ]
    stores = [
        pltpu.make_async_copy(send_ref.at[p], out_ref.at[:, p // 4, p % 4], out_sems.at[p])
        for p in range(prompts)
    ]
    for load in loads:
        load.start()
    valid = valid_ref[...].astype(jnp.float32).T
    for p in range(prompts):
        loads[p].wait()
        rows = in_ref[p]
        filled = jnp.where(valid[:, p : p + 1] > 0, rows.astype(jnp.float32), FILL).astype(rows.dtype)
        for h in range(2):
            for c in range(2):
                for place, index in enumerate((2 * h + c, 2 * (1 - h) + c)):
                    send_ref[p, h, c, :, place * quarter : (place + 1) * quarter] = filled[
                        :, index * quarter : (index + 1) * quarter
                    ]
        stores[p].start()
    for store in stores:
        store.wait()


def pack(embeddings, valid_mask):
    prompts, block_rows, features = embeddings.shape
    half = features // 2
    out = pl.pallas_call(
        pack_kernel,
        in_specs=[in_hbm(), whole()],
        out_specs=in_hbm(),
        out_shape=jax.ShapeDtypeStruct((2, 2, 4, 2, block_rows, half), embeddings.dtype),
        scratch_shapes=[
            pltpu.VMEM(embeddings.shape, embeddings.dtype),
            pltpu.VMEM((prompts, 2, 2, block_rows, half), embeddings.dtype),
            pltpu.SemaphoreType.DMA((prompts,)),
            pltpu.SemaphoreType.DMA((prompts,)),
        ],
    )(embeddings, valid_mask)
    return out.reshape(32, block_rows, half)


def weight_copies(place_ref, pieces, w_ref, sems, first, s):
    quarter = w_ref.shape[0]
    rows = quarter // 4
    position = lax.rem(place_ref[0] + s, 4)
    lanes = pl.multiple_of((position - first) * quarter, quarter)
    copies = []
    for index, (from_plane, from_row, half) in enumerate(PIECES):
        if from_plane == s:
            count = pieces[index].shape[0]
            at = pl.multiple_of(lax.rem(place_ref[1] + from_row, 4) * rows + half * count, count)
            target = w_ref.at[pl.ds(at, count), pl.ds(lanes, quarter)]
            copies.append(pltpu.make_async_copy(pieces[index], target, sems.at[index]))
    return jnp.logical_and(position >= first, position < first + 2), copies


def load_weights(place_ref, pieces, w_ref, sems, first):
    for s in range(4):
        here, copies = weight_copies(place_ref, pieces, w_ref, sems, first, s)

        @pl.when(here)
        def _():
            for copy in copies:
                copy.start()


def wait_weights(place_ref, pieces, w_ref, sems, first):
    for s in range(4):
        here, copies = weight_copies(place_ref, pieces, w_ref, sems, first, s)

        @pl.when(here)
        def _():
            for copy in copies:
                copy.wait()


def times_rows(w_ref, rows):
    return lax.dot_general(w_ref[...], rows, (((1,), (1,)), ((), ())), preferred_element_type=jnp.float32)


def row_loads(source, target, sems):
    rows = target.shape[0] // CHUNKS
    at = [pl.ds(n * rows, rows) for n in range(CHUNKS)]
    return [pltpu.make_async_copy(source.at[at[n]], target.at[at[n]], sems.at[n]) for n in range(CHUNKS)]


def near_kernel(place_ref, near_hbm, *refs):
    pieces, (mixed_hbm, w_ref, near_ref, mixed_ref, sems, near_sems, out_sems) = refs[:COUNT], refs[COUNT:]
    load_weights(place_ref, pieces, w_ref, sems, 0)
    loads = row_loads(near_hbm, near_ref, near_sems)
    for load in loads:
        load.start()
    wait_weights(place_ref, pieces, w_ref, sems, 0)
    rows = near_ref.shape[0] // CHUNKS
    stores = []
    for n in range(CHUNKS):
        loads[n].wait()
        mixed_ref[n] = times_rows(w_ref, near_ref[n * rows : (n + 1) * rows, :])
        stores.append(pltpu.make_async_copy(mixed_ref.at[n], mixed_hbm.at[n], out_sems.at[n]))
        stores[n].start()
    for store in stores:
        store.wait()


def far_kernel(place_ref, near_hbm, far_hbm, mixed_hbm, *refs):
    pieces, outs, scratch = refs[:COUNT], refs[COUNT : COUNT + 2], refs[COUNT + 2 :]
    kept_ref, given_ref = outs
    w_ref, far_ref, first_ref, mixed_ref, total_ref, table_ref, sems, far_sems, mixed_sems, first_sem = scratch
    load_weights(place_ref, pieces, w_ref, sems, 2)
    quarter = w_ref.shape[0]
    slots = table_ref.shape[0]
    rows = slots // CHUNKS
    loads = row_loads(far_hbm, far_ref, far_sems)
    partials = [pltpu.make_async_copy(mixed_hbm.at[n], mixed_ref.at[n], mixed_sems.at[n]) for n in range(CHUNKS)]
    first = pltpu.make_async_copy(near_hbm.at[:, pl.ds(0, quarter)], first_ref, first_sem.at[0])
    for n in range(CHUNKS):
        loads[n].start()
        partials[n].start()
    first.start()
    wait_weights(place_ref, pieces, w_ref, sems, 2)
    for n in range(CHUNKS):
        at = slice(n * rows, (n + 1) * rows)
        loads[n].wait()
        partials[n].wait()
        total_ref[:, at] = (mixed_ref[n] + times_rows(w_ref, far_ref[at, :])).astype(total_ref.dtype)
    first.wait()
    hidden = jnp.where(first_ref[:, :1].astype(jnp.float32) < FILL_TEST, 0.0, HIDDEN)
    table_ref[...] = jnp.dot(first_ref[...], total_ref[...], preferred_element_type=jnp.float32) + hidden
    c = place_ref[2]
    block = 128
    part = kept_ref.shape[1]
    groups = block // (2 * part)
    for i in range(slots // block):
        at = slice(i * block, (i + 1) * block)
        skew = table_ref[at, :] - table_ref[:, at].T
        skew = skew.reshape(groups, 2, part, slots)
        low, high = skew[:, 0], skew[:, 1]
        at = slice(i * groups, (i + 1) * groups)
        kept_ref[at] = jnp.where(c == 0, low, high).astype(kept_ref.dtype)
        given_ref[at] = jnp.where(c == 0, high, low).astype(given_ref.dtype)


def in_hbm():
    return pl.BlockSpec(memory_space=pl.ANY)


def whole():
    return pl.BlockSpec(memory_space=pltpu.VMEM)


def score_parts(place, near, far, pieces):
    slots, half = near.shape
    quarter = half // 2
    rows = slots // CHUNKS
    scalars = pl.BlockSpec(memory_space=pltpu.SMEM)
    limit = pltpu.CompilerParams(vmem_limit_bytes=56 * 2**20)
    four = pltpu.SemaphoreType.DMA((CHUNKS,))
    each = pltpu.SemaphoreType.DMA((COUNT,))
    mixed = pl.pallas_call(
        near_kernel,
        in_specs=[scalars] + [in_hbm()] * (COUNT + 1),
        out_specs=in_hbm(),
        out_shape=jax.ShapeDtypeStruct((CHUNKS, quarter, rows), jnp.float32),
        scratch_shapes=[
            pltpu.VMEM((quarter, half), near.dtype),
            pltpu.VMEM((slots, half), near.dtype),
            pltpu.VMEM((CHUNKS, quarter, rows), jnp.float32),
            each,
            four,
            four,
        ],
        compiler_params=limit,
        cost_estimate=pl.CostEstimate(
            flops=2 * quarter * half * slots, bytes_accessed=12 * 2**20, transcendentals=0
        ),
    )(place, near, *pieces)
    part = slots // 32
    return pl.pallas_call(
        far_kernel,
        in_specs=[scalars] + [in_hbm()] * (COUNT + 3),
        out_specs=[whole(), whole()],
        out_shape=[
            jax.ShapeDtypeStruct((16, part, slots), jnp.bfloat16),
            jax.ShapeDtypeStruct((16, part, slots), jnp.bfloat16),
        ],
        scratch_shapes=[
            pltpu.VMEM((quarter, half), near.dtype),
            pltpu.VMEM((slots, half), near.dtype),
            pltpu.VMEM((slots, quarter), near.dtype),
            pltpu.VMEM((CHUNKS, quarter, rows), jnp.float32),
            pltpu.VMEM((quarter, slots), near.dtype),
            pltpu.VMEM((slots, slots), jnp.float32),
            each,
            four,
            four,
            pltpu.SemaphoreType.DMA((1,)),
        ],
        compiler_params=limit,
        cost_estimate=pl.CostEstimate(
            flops=2 * quarter * (half + slots) * slots, bytes_accessed=16 * 2**20, transcendentals=0
        ),
    )(place, near, far, mixed, *pieces)


def scored(embeddings, head_weight, valid_mask):
    prompts, block_rows, features = embeddings.shape
    quarter = features // 4
    slots = 32 * block_rows
    x = lax.axis_index("x")
    y = lax.axis_index("y")
    z = lax.axis_index("z")
    c = lax.axis_index("c")

    slab = lax.dynamic_slice_in_dim(head_weight, (y ^ ((x % 2) * 2 + x // 2)) * quarter, quarter, 1)
    part_a = lax.ppermute(slab, ("y", "c"), slab_pairs(0))
    part_b = lax.ppermute(slab, ("y", "c"), slab_pairs(1))
    outgoing = pack(embeddings, valid_mask)
    at_home = c == y % 2
    own = jnp.concatenate([jnp.where(at_home, part_a, part_b), jnp.where(at_home, part_b, part_a)])
    chain = [own]
    for step in (-1, 2, 1):
        chain.append(ring(own, "z", step))
    near = lax.all_to_all(outgoing, RESP_AXES, 0, 0, tiled=True).reshape(slots, 2 * quarter)
    below, above = [], []
    for piece in chain:
        below.append(ring(piece, "x", 1))
        above.append(ring(piece, "x", -1))
    across = []
    for index, steps in enumerate(((1,), (-1,), (1, -1), (1,))):
        for half, step in enumerate(steps):
            piece = (below if step == 1 else above)[index]
            rows = piece.shape[0] // len(steps)
            across.append(ring(piece[half * rows : (half + 1) * rows], "x", step))
    far = swap_cores(near)

    place = jnp.stack([x, z, c]).astype(jnp.int32)
    kept, given = score_parts(place, near, far, [*chain, *above, *below, *across])
    half_scores = (kept.astype(jnp.float32) + swap_cores(given).astype(jnp.float32)).astype(jnp.bfloat16)
    returned = lax.all_to_all(half_scores, ("y", "z"), 0, 0, tiled=True).astype(jnp.float32)
    scores = returned[:prompts] + returned[prompts:]

    valid_rows = valid_mask.astype(jnp.float32)
    counts = jnp.sum((scores > HIDDEN_TEST).astype(jnp.float32), axis=2)
    preferences = jax.nn.sigmoid(scores) * valid_rows[:, :, None]
    totals = jnp.sum(preferences, axis=2) - 0.5 * valid_rows
    win_rates = valid_rows * totals / jnp.maximum(counts - 1.0, 1.0)
    return preferences, win_rates


def solution(mesh):
    mesh = Mesh(mesh.devices.reshape(4, 4, 4, 2), ("x", "y", "z", "c"))
    spec = P("x", RESP_AXES)
    return jax.shard_map(
        scored,
        mesh=mesh,
        in_specs=(P("x", RESP_AXES, None), P(RESP_AXES, None), spec),
        out_specs=(P("x", RESP_AXES, None), spec),
        check_vma=False,
    )
```

```python
import jax
import jax.numpy as jnp
from jax import lax
from jax.experimental import pallas as pl
from jax.experimental.pallas import tpu as pltpu
from jax.sharding import Mesh, PartitionSpec as P


RESP_AXES = ("y", "z", "c")
FILL = 256.0
FILL_TEST = 128.0
HIDDEN = 1e30
HIDDEN_TEST = -1e29
CHUNKS = 2
PIECES = tuple((s, r, 0) for s in (0, 1, 3) for r in range(4)) + ((2, 0, 0), (2, 1, 0), (2, 2, 0), (2, 2, 1), (2, 3, 0))
COUNT = len(PIECES)


def ring(value, axis, step):
    return lax.ppermute(value, axis, [(i, (i + step) % 4) for i in range(4)])


def swap_cores(value):
    return lax.ppermute(value, "c", [(0, 1), (1, 0)])


def slab_pairs(first_core):
    pairs = []
    for y in range(4):
        for c in range(2):
            target = y if c == first_core else y ^ 1
            pairs.append((y * 2 + c, target * 2 + y % 2))
    return pairs


def pack_kernel(rows_ref, valid_ref, out_ref, in_ref, send_ref, in_sems, out_sems):
    prompts, _, features = in_ref.shape
    half = features // 2
    quarter = half // 2
    loads = [
        pltpu.make_async_copy(rows_ref.at[p], in_ref.at[p], in_sems.at[p]) for p in range(prompts)
    ]
    stores = [
        pltpu.make_async_copy(send_ref.at[p], out_ref.at[:, p // 4, p % 4], out_sems.at[p])
        for p in range(prompts)
    ]
    for load in loads:
        load.start()
    valid = valid_ref[...].astype(jnp.float32).T
    for p in range(prompts):
        loads[p].wait()
        rows = in_ref[p]
        filled = jnp.where(valid[:, p : p + 1] > 0, rows.astype(jnp.float32), FILL).astype(rows.dtype)
        for h in range(2):
            for c in range(2):
                for place, index in enumerate((2 * h + c, 2 * (1 - h) + c)):
                    send_ref[p, h, c, :, place * quarter : (place + 1) * quarter] = filled[
                        :, index * quarter : (index + 1) * quarter
                    ]
        stores[p].start()
    for store in stores:
        store.wait()


def pack(embeddings, valid_mask):
    prompts, block_rows, features = embeddings.shape
    half = features // 2
    out = pl.pallas_call(
        pack_kernel,
        in_specs=[in_hbm(), whole()],
        out_specs=in_hbm(),
        out_shape=jax.ShapeDtypeStruct((2, 2, 4, 2, block_rows, half), embeddings.dtype),
        scratch_shapes=[
            pltpu.VMEM(embeddings.shape, embeddings.dtype),
            pltpu.VMEM((prompts, 2, 2, block_rows, half), embeddings.dtype),
            pltpu.SemaphoreType.DMA((prompts,)),
            pltpu.SemaphoreType.DMA((prompts,)),
        ],
    )(embeddings, valid_mask)
    return out.reshape(32, block_rows, half)


def weight_copies(place_ref, pieces, w_ref, sems, first, s):
    quarter = w_ref.shape[0]
    rows = quarter // 4
    position = lax.rem(place_ref[0] + s, 4)
    lanes = pl.multiple_of((position - first) * quarter, quarter)
    copies = []
    for index, (from_plane, from_row, half) in enumerate(PIECES):
        if from_plane == s:
            count = pieces[index].shape[0]
            at = pl.multiple_of(lax.rem(place_ref[1] + from_row, 4) * rows + half * count, count)
            target = w_ref.at[pl.ds(at, count), pl.ds(lanes, quarter)]
            copies.append(pltpu.make_async_copy(pieces[index], target, sems.at[index]))
    return jnp.logical_and(position >= first, position < first + 2), copies


def load_weights(place_ref, pieces, w_ref, sems, first):
    for s in range(4):
        here, copies = weight_copies(place_ref, pieces, w_ref, sems, first, s)

        @pl.when(here)
        def _():
            for copy in copies:
                copy.start()


def wait_weights(place_ref, pieces, w_ref, sems, first):
    for s in range(4):
        here, copies = weight_copies(place_ref, pieces, w_ref, sems, first, s)

        @pl.when(here)
        def _():
            for copy in copies:
                copy.wait()


def times_rows(w_ref, rows):
    return lax.dot_general(w_ref[...], rows, (((1,), (1,)), ((), ())), preferred_element_type=jnp.float32)


def row_loads(source, target, sems):
    rows = target.shape[0] // CHUNKS
    at = [pl.ds(n * rows, rows) for n in range(CHUNKS)]
    return [pltpu.make_async_copy(source.at[at[n]], target.at[at[n]], sems.at[n]) for n in range(CHUNKS)]


def near_kernel(place_ref, near_hbm, *refs):
    pieces, (mixed_ref, w_ref, near_ref, sems, near_sems) = refs[:COUNT], refs[COUNT:]
    load_weights(place_ref, pieces, w_ref, sems, 0)
    loads = row_loads(near_hbm, near_ref, near_sems)
    for load in loads:
        load.start()
    wait_weights(place_ref, pieces, w_ref, sems, 0)
    rows = near_ref.shape[0] // CHUNKS
    for n in range(CHUNKS):
        loads[n].wait()
        mixed_ref[n] = times_rows(w_ref, near_ref[n * rows : (n + 1) * rows, :])


def far_kernel(place_ref, near_hbm, far_hbm, mixed_ref, *refs):
    pieces, outs, scratch = refs[:COUNT], refs[COUNT : COUNT + 2], refs[COUNT + 2 :]
    kept_ref, given_ref = outs
    w_ref, far_ref, first_ref, total_ref, table_ref, sems, far_sems, first_sem = scratch
    load_weights(place_ref, pieces, w_ref, sems, 2)
    quarter = w_ref.shape[0]
    slots = table_ref.shape[0]
    rows = slots // CHUNKS
    loads = row_loads(far_hbm, far_ref, far_sems)
    first = pltpu.make_async_copy(near_hbm.at[:, pl.ds(0, quarter)], first_ref, first_sem.at[0])
    for n in range(CHUNKS):
        loads[n].start()
    first.start()
    wait_weights(place_ref, pieces, w_ref, sems, 2)
    for n in range(CHUNKS):
        at = slice(n * rows, (n + 1) * rows)
        loads[n].wait()
        total_ref[:, at] = (mixed_ref[n] + times_rows(w_ref, far_ref[at, :])).astype(total_ref.dtype)
    first.wait()
    hidden = jnp.where(first_ref[:, :1].astype(jnp.float32) < FILL_TEST, 0.0, HIDDEN)
    table_ref[...] = jnp.dot(first_ref[...], total_ref[...], preferred_element_type=jnp.float32) + hidden
    c = place_ref[2]
    block = 128
    part = kept_ref.shape[1]
    groups = block // (2 * part)
    for i in range(slots // block):
        at = slice(i * block, (i + 1) * block)
        skew = table_ref[at, :] - table_ref[:, at].T
        skew = skew.reshape(groups, 2, part, slots)
        low, high = skew[:, 0], skew[:, 1]
        at = slice(i * groups, (i + 1) * groups)
        kept_ref[at] = jnp.where(c == 0, low, high).astype(kept_ref.dtype)
        given_ref[at] = jnp.where(c == 0, high, low).astype(given_ref.dtype)


def in_hbm():
    return pl.BlockSpec(memory_space=pl.ANY)


def whole():
    return pl.BlockSpec(memory_space=pltpu.VMEM)


def score_parts(place, near, far, pieces):
    slots, half = near.shape
    quarter = half // 2
    rows = slots // CHUNKS
    scalars = pl.BlockSpec(memory_space=pltpu.SMEM)
    four = pltpu.SemaphoreType.DMA((CHUNKS,))
    each = pltpu.SemaphoreType.DMA((COUNT,))
    mixed = pl.pallas_call(
        near_kernel,
        in_specs=[scalars] + [in_hbm()] * (COUNT + 1),
        out_specs=whole(),
        out_shape=pltpu.VMEM((CHUNKS, quarter, rows), jnp.float32),
        scratch_shapes=[
            pltpu.VMEM((quarter, half), near.dtype),
            pltpu.VMEM((slots, half), near.dtype),
            each,
            four,
        ],
        compiler_params=pltpu.CompilerParams(vmem_limit_bytes=16 * 2**20),
        cost_estimate=pl.CostEstimate(
            flops=2 * quarter * half * slots, bytes_accessed=12 * 2**20, transcendentals=0
        ),
    )(place, near, *pieces)
    part = slots // 32
    return pl.pallas_call(
        far_kernel,
        in_specs=[scalars, in_hbm(), in_hbm(), whole()] + [in_hbm()] * COUNT,
        out_specs=[whole(), whole()],
        out_shape=[
            pltpu.VMEM((16, part, slots), jnp.bfloat16),
            pltpu.VMEM((16, part, slots), jnp.bfloat16),
        ],
        scratch_shapes=[
            pltpu.VMEM((quarter, half), near.dtype),
            pltpu.VMEM((slots, half), near.dtype),
            pltpu.VMEM((slots, quarter), near.dtype),
            pltpu.VMEM((quarter, slots), near.dtype),
            pltpu.VMEM((slots, slots), jnp.float32),
            each,
            four,
            pltpu.SemaphoreType.DMA((1,)),
        ],
        compiler_params=pltpu.CompilerParams(vmem_limit_bytes=32 * 2**20),
        cost_estimate=pl.CostEstimate(
            flops=2 * quarter * (half + slots) * slots, bytes_accessed=16 * 2**20, transcendentals=0
        ),
    )(place, near, far, mixed, *pieces)


def scored(embeddings, head_weight, valid_mask):
    prompts, block_rows, features = embeddings.shape
    quarter = features // 4
    slots = 32 * block_rows
    x = lax.axis_index("x")
    y = lax.axis_index("y")
    z = lax.axis_index("z")
    c = lax.axis_index("c")

    slab = lax.dynamic_slice_in_dim(head_weight, (y ^ ((x % 2) * 2 + x // 2)) * quarter, quarter, 1)
    part_a = lax.ppermute(slab, ("y", "c"), slab_pairs(0))
    part_b = lax.ppermute(slab, ("y", "c"), slab_pairs(1))
    outgoing = pack(embeddings, valid_mask)
    at_home = c == y % 2
    own = jnp.concatenate([jnp.where(at_home, part_a, part_b), jnp.where(at_home, part_b, part_a)])
    chain = [own]
    for step in (-1, 2, 1):
        chain.append(ring(own, "z", step))
    near = lax.all_to_all(outgoing, RESP_AXES, 0, 0, tiled=True).reshape(slots, 2 * quarter)
    below, above = [], []
    for piece in chain:
        below.append(ring(piece, "x", 1))
        above.append(ring(piece, "x", -1))
    across = []
    for index, steps in enumerate(((1,), (-1,), (1, -1), (1,))):
        for half, step in enumerate(steps):
            piece = (below if step == 1 else above)[index]
            rows = piece.shape[0] // len(steps)
            across.append(ring(piece[half * rows : (half + 1) * rows], "x", step))
    far = swap_cores(near)

    place = jnp.stack([x, z, c]).astype(jnp.int32)
    kept, given = score_parts(place, near, far, [*chain, *above, *below, *across])
    half_scores = (kept.astype(jnp.float32) + swap_cores(given).astype(jnp.float32)).astype(jnp.bfloat16)
    returned = lax.all_to_all(half_scores, ("y", "z"), 0, 0, tiled=True).astype(jnp.float32)
    scores = returned[:prompts] + returned[prompts:]

    valid_rows = valid_mask.astype(jnp.float32)
    counts = jnp.sum((scores > HIDDEN_TEST).astype(jnp.float32), axis=2)
    preferences = jax.nn.sigmoid(scores) * valid_rows[:, :, None]
    totals = jnp.sum(preferences, axis=2) - 0.5 * valid_rows
    win_rates = valid_rows * totals / jnp.maximum(counts - 1.0, 1.0)
    return preferences, win_rates


def solution(mesh):
    mesh = Mesh(mesh.devices.reshape(4, 4, 4, 2), ("x", "y", "z", "c"))
    spec = P("x", RESP_AXES)
    return jax.shard_map(
        scored,
        mesh=mesh,
        in_specs=(P("x", RESP_AXES, None), P(RESP_AXES, None), spec),
        out_specs=(P("x", RESP_AXES, None), spec),
        check_vma=False,
    )
```

```python
import jax
import jax.numpy as jnp
from jax import lax
from jax.experimental import pallas as pl
from jax.experimental.pallas import tpu as pltpu
from jax.sharding import Mesh, PartitionSpec as P


RESP_AXES = ("y", "z", "c")
FILL = 256.0
FILL_TEST = 128.0
HIDDEN = 1e30
HIDDEN_TEST = -1e29
CHUNKS = 2
PIECES = tuple((s, r, 0) for s in (0, 1, 3) for r in range(4)) + ((2, 0, 0), (2, 1, 0), (2, 2, 0), (2, 2, 1), (2, 3, 0))
COUNT = len(PIECES)


def ring(value, axis, step):
    return lax.ppermute(value, axis, [(i, (i + step) % 4) for i in range(4)])


def swap_cores(value):
    return lax.ppermute(value, "c", [(0, 1), (1, 0)])


def slab_pairs(first_core):
    pairs = []
    for y in range(4):
        for c in range(2):
            target = y if c == first_core else y ^ 1
            pairs.append((y * 2 + c, target * 2 + y % 2))
    return pairs


def pack_kernel(rows_ref, valid_ref, out_ref, in_ref, send_ref, in_sems, out_sems):
    prompts, _, features = in_ref.shape
    half = features // 2
    quarter = half // 2
    loads = [
        pltpu.make_async_copy(rows_ref.at[p], in_ref.at[p], in_sems.at[p]) for p in range(prompts)
    ]
    stores = [
        pltpu.make_async_copy(send_ref.at[p], out_ref.at[:, p // 4, p % 4], out_sems.at[p])
        for p in range(prompts)
    ]
    for load in loads:
        load.start()
    valid = valid_ref[...].astype(jnp.float32).T
    for p in range(prompts):
        loads[p].wait()
        rows = in_ref[p]
        filled = jnp.where(valid[:, p : p + 1] > 0, rows.astype(jnp.float32), FILL).astype(rows.dtype)
        for h in range(2):
            for c in range(2):
                for place, index in enumerate((2 * h + c, 2 * (1 - h) + c)):
                    send_ref[p, h, c, :, place * quarter : (place + 1) * quarter] = filled[
                        :, index * quarter : (index + 1) * quarter
                    ]
        stores[p].start()
    for store in stores:
        store.wait()


def pack(embeddings, valid_mask):
    prompts, block_rows, features = embeddings.shape
    half = features // 2
    out = pl.pallas_call(
        pack_kernel,
        in_specs=[in_hbm(), whole()],
        out_specs=in_hbm(),
        out_shape=jax.ShapeDtypeStruct((2, 2, 4, 2, block_rows, half), embeddings.dtype),
        scratch_shapes=[
            pltpu.VMEM(embeddings.shape, embeddings.dtype),
            pltpu.VMEM((prompts, 2, 2, block_rows, half), embeddings.dtype),
            pltpu.SemaphoreType.DMA((prompts,)),
            pltpu.SemaphoreType.DMA((prompts,)),
        ],
    )(embeddings, valid_mask)
    return out.reshape(32, block_rows, half)


def weight_copies(place_ref, pieces, w_ref, sems, first, s):
    quarter = w_ref.shape[0]
    rows = quarter // 4
    position = lax.rem(place_ref[0] + s, 4)
    lanes = pl.multiple_of((position - first) * quarter, quarter)
    copies = []
    for index, (from_plane, from_row, half) in enumerate(PIECES):
        if from_plane == s:
            count = pieces[index].shape[0]
            at = pl.multiple_of(lax.rem(place_ref[1] + from_row, 4) * rows + half * count, count)
            target = w_ref.at[pl.ds(at, count), pl.ds(lanes, quarter)]
            copies.append(pltpu.make_async_copy(pieces[index], target, sems.at[index]))
    return jnp.logical_and(position >= first, position < first + 2), copies


def load_weights(place_ref, pieces, w_ref, sems, first):
    for s in range(4):
        here, copies = weight_copies(place_ref, pieces, w_ref, sems, first, s)

        @pl.when(here)
        def _():
            for copy in copies:
                copy.start()


def wait_weights(place_ref, pieces, w_ref, sems, first):
    for s in range(4):
        here, copies = weight_copies(place_ref, pieces, w_ref, sems, first, s)

        @pl.when(here)
        def _():
            for copy in copies:
                copy.wait()


def times_rows(w_ref, rows):
    return lax.dot_general(w_ref[...], rows, (((1,), (1,)), ((), ())), preferred_element_type=jnp.float32)


def row_loads(source, target, sems):
    rows = target.shape[0] // CHUNKS
    at = [pl.ds(n * rows, rows) for n in range(CHUNKS)]
    return [pltpu.make_async_copy(source.at[at[n]], target.at[at[n]], sems.at[n]) for n in range(CHUNKS)]


def near_kernel(place_ref, near_hbm, *refs):
    pieces, (mixed_ref, w_ref, near_ref, sems, near_sems) = refs[:COUNT], refs[COUNT:]
    load_weights(place_ref, pieces, w_ref, sems, 0)
    loads = row_loads(near_hbm, near_ref, near_sems)
    for load in loads:
        load.start()
    wait_weights(place_ref, pieces, w_ref, sems, 0)
    rows = near_ref.shape[0] // CHUNKS
    for n in range(CHUNKS):
        loads[n].wait()
        mixed_ref[n] = times_rows(w_ref, near_ref[n * rows : (n + 1) * rows, :])


def far_kernel(place_ref, near_hbm, far_hbm, mixed_ref, *refs):
    pieces, outs, scratch = refs[:COUNT], refs[COUNT : COUNT + 2], refs[COUNT + 2 :]
    kept_ref, given_ref = outs
    w_ref, far_ref, first_ref, total_ref, table_ref, sems, far_sems, first_sem = scratch
    load_weights(place_ref, pieces, w_ref, sems, 2)
    quarter = w_ref.shape[0]
    slots = table_ref.shape[0]
    rows = slots // CHUNKS
    loads = row_loads(far_hbm, far_ref, far_sems)
    first = pltpu.make_async_copy(near_hbm.at[:, pl.ds(0, quarter)], first_ref, first_sem.at[0])
    for n in range(CHUNKS):
        loads[n].start()
    first.start()
    wait_weights(place_ref, pieces, w_ref, sems, 2)
    for n in range(CHUNKS):
        at = slice(n * rows, (n + 1) * rows)
        loads[n].wait()
        total_ref[:, at] = (mixed_ref[n] + times_rows(w_ref, far_ref[at, :])).astype(total_ref.dtype)
    first.wait()
    hidden = jnp.where(first_ref[:, :1].astype(jnp.float32) < FILL_TEST, 0.0, HIDDEN)
    table_ref[...] = jnp.dot(first_ref[...], total_ref[...], preferred_element_type=jnp.float32) + hidden
    c = place_ref[2]
    block = 128
    part = kept_ref.shape[1]
    groups = block // (2 * part)
    for i in range(slots // block):
        at = slice(i * block, (i + 1) * block)
        skew = table_ref[at, :] - table_ref[:, at].T
        skew = skew.reshape(groups, 2, part, slots)
        low, high = skew[:, 0], skew[:, 1]
        at = slice(i * groups, (i + 1) * groups)
        kept_ref[at] = jnp.where(c == 0, low, high).astype(kept_ref.dtype)
        given_ref[at] = jnp.where(c == 0, high, low).astype(given_ref.dtype)


def in_hbm():
    return pl.BlockSpec(memory_space=pl.ANY)


def whole():
    return pl.BlockSpec(memory_space=pltpu.VMEM)


def score_parts(place, near, far, pieces):
    slots, half = near.shape
    quarter = half // 2
    rows = slots // CHUNKS
    scalars = pl.BlockSpec(memory_space=pltpu.SMEM)
    four = pltpu.SemaphoreType.DMA((CHUNKS,))
    each = pltpu.SemaphoreType.DMA((COUNT,))
    mixed = pl.pallas_call(
        near_kernel,
        in_specs=[scalars] + [in_hbm()] * (COUNT + 1),
        out_specs=whole(),
        out_shape=pltpu.VMEM((CHUNKS, quarter, rows), jnp.float32),
        scratch_shapes=[
            pltpu.VMEM((quarter, half), near.dtype),
            pltpu.VMEM((slots, half), near.dtype),
            each,
            four,
        ],
        compiler_params=pltpu.CompilerParams(vmem_limit_bytes=12 * 2**20),
        cost_estimate=pl.CostEstimate(
            flops=2 * quarter * half * slots, bytes_accessed=12 * 2**20, transcendentals=0
        ),
    )(place, near, *pieces)
    part = slots // 32
    return pl.pallas_call(
        far_kernel,
        in_specs=[scalars, in_hbm(), in_hbm(), whole()] + [in_hbm()] * COUNT,
        out_specs=[whole(), whole()],
        out_shape=[
            pltpu.VMEM((16, part, slots), jnp.bfloat16),
            pltpu.VMEM((16, part, slots), jnp.bfloat16),
        ],
        scratch_shapes=[
            pltpu.VMEM((quarter, half), near.dtype),
            pltpu.VMEM((slots, half), near.dtype),
            pltpu.VMEM((slots, quarter), near.dtype),
            pltpu.VMEM((quarter, slots), near.dtype),
            pltpu.VMEM((slots, slots), jnp.float32),
            each,
            four,
            pltpu.SemaphoreType.DMA((1,)),
        ],
        compiler_params=pltpu.CompilerParams(vmem_limit_bytes=24 * 2**20),
        cost_estimate=pl.CostEstimate(
            flops=2 * quarter * (half + slots) * slots, bytes_accessed=16 * 2**20, transcendentals=0
        ),
    )(place, near, far, mixed, *pieces)


def scored(embeddings, head_weight, valid_mask):
    prompts, block_rows, features = embeddings.shape
    quarter = features // 4
    slots = 32 * block_rows
    x = lax.axis_index("x")
    y = lax.axis_index("y")
    z = lax.axis_index("z")
    c = lax.axis_index("c")

    slab = lax.dynamic_slice_in_dim(head_weight, (y ^ ((x % 2) * 2 + x // 2)) * quarter, quarter, 1)
    part_a = lax.ppermute(slab, ("y", "c"), slab_pairs(0))
    part_b = lax.ppermute(slab, ("y", "c"), slab_pairs(1))
    outgoing = pack(embeddings, valid_mask)
    at_home = c == y % 2
    own = jnp.where(at_home, jnp.concatenate([part_a, part_b]), jnp.concatenate([part_b, part_a]))
    chain = [own]
    for step in (-1, 2, 1):
        chain.append(ring(own, "z", step))
    near = lax.all_to_all(outgoing, RESP_AXES, 0, 0, tiled=True).reshape(slots, 2 * quarter)
    below, above = [], []
    for piece in chain:
        below.append(ring(piece, "x", 1))
        above.append(ring(piece, "x", -1))
    across = []
    for index, steps in enumerate(((1,), (-1,), (1, -1), (1,))):
        for half, step in enumerate(steps):
            piece = (below if step == 1 else above)[index]
            rows = piece.shape[0] // len(steps)
            across.append(ring(piece[half * rows : (half + 1) * rows], "x", step))
    far = swap_cores(near)

    place = jnp.stack([x, z, c]).astype(jnp.int32)
    kept, given = score_parts(place, near, far, [*chain, *above, *below, *across])
    half_scores = (kept.astype(jnp.float32) + swap_cores(given).astype(jnp.float32)).astype(jnp.bfloat16)
    returned = lax.all_to_all(half_scores, ("y", "z"), 0, 0, tiled=True).astype(jnp.float32)
    scores = returned[:prompts] + returned[prompts:]

    valid_rows = valid_mask.astype(jnp.float32)
    counts = jnp.sum((scores > HIDDEN_TEST).astype(jnp.float32), axis=2)
    preferences = jax.nn.sigmoid(scores) * valid_rows[:, :, None]
    totals = jnp.sum(preferences, axis=2) - 0.5 * valid_rows
    win_rates = valid_rows * totals / jnp.maximum(counts - 1.0, 1.0)
    return preferences, win_rates


def solution(mesh):
    mesh = Mesh(mesh.devices.reshape(4, 4, 4, 2), ("x", "y", "z", "c"))
    spec = P("x", RESP_AXES)
    return jax.shard_map(
        scored,
        mesh=mesh,
        in_specs=(P("x", RESP_AXES, None), P(RESP_AXES, None), spec),
        out_specs=(P("x", RESP_AXES, None), spec),
        check_vma=False,
    )
```
